32 devices in a mesh: expert: 4 (over y, core), unit: 8 (over z, x).
Axes of the slice: x: 2, y: 2, z: 4, core: 2. Of those that a mesh axis runs over, the one named last changes fastest.
Arguments:
- a_gate: bfloat16 [4, 14336, 4096], P('expert', 'unit'), may hold values from -0.09375 to 0.09375
- a_up: bfloat16 [4, 14336, 4096], P('expert', 'unit'), may hold values from -0.09375 to 0.09375
- b_gate: bfloat16 [4, 14336, 4096], P('expert', 'unit'), may hold values from -0.09375 to 0.09375
- b_up: bfloat16 [4, 14336, 4096], P('expert', 'unit'), may hold values from -0.09375 to 0.09375
- order: int32 [4, 448], P('expert'), may hold values from 0 to 447, each once within a row
- calib: bfloat16 [128, 4096], P(('expert', 'unit')), may hold values from -6 to 6
Outputs:
- merged_gate: bfloat16 [4, 14336, 4096], P('expert', 'unit')
- merged_up: bfloat16 [4, 14336, 4096], P('expert', 'unit')
- hidden: bfloat16 [4, 14336, 128], P('expert', 'unit')
The draws below stay inside these ranges and needn't reach their ends.
Inputs may be any that keep to these rules, and one draw needn't show every extreme that they name: Each row of order is a permutation of the 448 block numbers.
All inputs are finite; a program needn't handle non-finite values.
Results may differ from the reference program's by a relative error of at most 0.006.
Values may be sent and summed in bfloat16 or wider, within the bound.
A program may use at most 256 MiB of HBM per device.

```python
import jax
import jax.numpy as jnp
from jax import lax

D = 4096
FF = 14336
BLOCK = 32
EXPERTS = 4
NBLOCKS = 448
TOKENS = 128


def steps_of(key, shape, pieces, smallest, largest):
    def one(position, parts):
        draws = jax.random.uniform(jax.random.fold_in(jax.random.fold_in(key, 6), position), (parts,), jnp.float32, smallest / len(pieces), largest / len(pieces))
        return jnp.repeat(jnp.exp(draws), shape[position] // parts).reshape((-1,) + (1,) * (len(shape) - position - 1))

    loudness = one(*pieces[0])
    for cut in pieces[1:]:
        loudness = loudness * one(*cut)
    return loudness


def gaussian(stream_key, shape, scale, reach, split=(), held_as=jnp.bfloat16):
    loudness = steps_of(stream_key, shape, split, -0.22, 0.18) if split else 1.0
    values = jax.random.normal(stream_key, shape, jnp.float32) * scale * loudness
    return jnp.minimum(jnp.maximum(values, -reach), reach).astype(held_as)


def setup_inputs(seed: int = 0) -> dict:
    seeds = jax.random.split(jax.random.key(seed), 7)
    return {
        "a_gate": gaussian(seeds[0], (EXPERTS, FF, D), D ** -0.5, 0.09375, ((0, 4), (1, 8))),
        "a_up": gaussian(seeds[1], (EXPERTS, FF, D), D ** -0.5, 0.09375, ((0, 4), (1, 8))),
        "b_gate": gaussian(seeds[2], (EXPERTS, FF, D), D ** -0.5, 0.09375, ((0, 4), (1, 8))),
        "b_up": gaussian(seeds[3], (EXPERTS, FF, D), D ** -0.5, 0.09375, ((0, 4), (1, 8))),
        "order": jax.vmap(lambda own: jax.random.permutation(own, NBLOCKS))(jax.random.split(seeds[4], EXPERTS)).reshape((EXPERTS, NBLOCKS)).astype(jnp.int32),
        "calib": gaussian(seeds[5], (TOKENS, D), 1.0, 6.0, ((0, 32),)),
    }


def merge_one(items):
    gate_a, up_a, gate_b, up_b, dest, calib = items
    inverse = jnp.zeros((NBLOCKS,), jnp.int32).at[dest].set(jnp.arange(NBLOCKS, dtype=jnp.int32))
    moved_gate = jnp.take(gate_b.reshape(NBLOCKS, BLOCK, D), inverse, axis=0).reshape(FF, D)
    moved_up = jnp.take(up_b.reshape(NBLOCKS, BLOCK, D), inverse, axis=0).reshape(FF, D)
    merged_gate = ((gate_a.astype(jnp.float32) + moved_gate.astype(jnp.float32)) * 0.5).astype(jnp.bfloat16)
    merged_up = ((up_a.astype(jnp.float32) + moved_up.astype(jnp.float32)) * 0.5).astype(jnp.bfloat16)
    gate_pre = jnp.dot(merged_gate, calib.T, preferred_element_type=jnp.float32)
    up_pre = jnp.dot(merged_up, calib.T, preferred_element_type=jnp.float32)
    hidden = (jax.nn.silu(gate_pre) * up_pre).astype(jnp.bfloat16)
    return merged_gate, merged_up, hidden


def reference(a_gate, a_up, b_gate, b_up, order, calib):
    shared = jnp.broadcast_to(calib[None], (EXPERTS,) + calib.shape)
    merged_gate, merged_up, hidden = lax.map(merge_one, (a_gate, a_up, b_gate, b_up, order, shared))
    return merged_gate, merged_up, hidden
```

```python
import functools

import jax
import jax.numpy as jnp
from jax import lax
from jax.experimental import pallas as pl
from jax.experimental.pallas import tpu as pltpu
from jax.sharding import PartitionSpec as P

BLOCK = 32


def merge_kernel(ways, a_ref, r_ref, calib_ref, m_ref, pre_ref):
    wide = a_ref.shape[1] // ways
    total = None
    for way in range(ways):
        columns = slice(way * wide, (way + 1) * wide)
        merged = (
            (a_ref[:, columns].astype(jnp.float32) + r_ref[way].astype(jnp.float32)) * 0.5
        ).astype(jnp.bfloat16)
        m_ref[:, columns] = merged
        term = lax.dot_general(
            merged, calib_ref[:, columns], (((1,), (1,)), ((), ())), preferred_element_type=jnp.float32
        )
        total = term if total is None else total + term
    pre_ref[...] = total


def merge_xla(a, returned, calib):
    rows, width = a.shape
    returned = jnp.swapaxes(returned, 0, 1).reshape(rows, width)
    merged = ((a.astype(jnp.float32) + returned.astype(jnp.float32)) * 0.5).astype(jnp.bfloat16)
    pre = lax.dot_general(merged, calib, (((1,), (1,)), ((), ())), preferred_element_type=jnp.float32)
    return merged, pre


def merge(a, returned, calib):
    ways, rows, wide = returned.shape
    tokens, width = calib.shape
    if wide % 128:
        return merge_xla(a, returned, calib)
    tile = next(t for t in (256, 224, 128, 64, 32) if rows % t == 0)
    return pl.pallas_call(
        functools.partial(merge_kernel, ways),
        grid=(rows // tile,),
        in_specs=[
            pl.BlockSpec((tile, width), lambda i: (i, 0)),
            pl.BlockSpec((ways, tile, wide), lambda i: (0, i, 0)),
            pl.BlockSpec((tokens, width), lambda i: (0, 0)),
        ],
        out_specs=[
            pl.BlockSpec((tile, width), lambda i: (i, 0)),
            pl.BlockSpec((tile, tokens), lambda i: (i, 0)),
        ],
        out_shape=[
            jax.ShapeDtypeStruct((rows, width), jnp.bfloat16),
            jax.ShapeDtypeStruct((rows, tokens), jnp.float32),
        ],
        compiler_params=pltpu.CompilerParams(vmem_limit_bytes=40 * 1024 * 1024),
        cost_estimate=pl.CostEstimate(
            flops=2 * rows * width * tokens, bytes_accessed=6 * rows * width, transcendentals=0
        ),
    )(a, returned, calib)


def local(a_gate, a_up, b_gate, b_up, order, calib):
    blocks = order.shape[1]
    ways = lax.axis_size("unit")
    inverse = jnp.zeros((blocks,), jnp.int32).at[order[0]].set(jnp.arange(blocks, dtype=jnp.int32))
    everyone = lax.all_gather(calib, ("expert", "unit"), axis=0, tiled=True)

    def columns_of(b):
        rows, width = b.shape
        return jnp.swapaxes(b.reshape(rows, ways, width // ways), 0, 1)

    def relocate(columns):
        _, rows, wide = columns.shape
        grouped = columns.reshape(blocks, BLOCK, wide)
        return jnp.take(grouped, inverse, axis=0, mode="clip").reshape(ways, rows, wide)

    def bring(columns):
        return lax.all_to_all(columns, "unit", split_axis=0, concat_axis=0, tiled=True)

    gate = bring(columns_of(b_gate[0]))
    up_columns, everyone = lax.optimization_barrier((columns_of(b_up[0]), everyone))
    up = bring(up_columns)
    gate = bring(relocate(gate))
    up = bring(relocate(up))
    merged_gate, gate_pre = merge(a_gate[0], gate, everyone)
    merged_up, up_pre = merge(a_up[0], up, everyone)
    hidden = (jax.nn.silu(gate_pre) * up_pre).astype(jnp.bfloat16)
    return (merged_gate[None], merged_up[None], hidden[None])


def solution(mesh):
    in_specs = (
        P("expert", "unit", None),
        P("expert", "unit", None),
        P("expert", "unit", None),
        P("expert", "unit", None),
        P("expert", None),
        P(("expert", "unit"), None),
    )
    out_specs = (P("expert", "unit", None), P("expert", "unit", None), P("expert", "unit", None))
    return jax.shard_map(local, mesh=mesh, in_specs=in_specs, out_specs=out_specs, check_vma=False)
```
